256 devices in a mesh: sub: 32 (over z, x_lo, core), row: 8 (over y, x_hi).
Axes of the slice: x: 4 (x_hi: 2, x_lo: 2; x = x_hi * 2 + x_lo), y: 4, z: 8, core: 2. Of those that a mesh axis runs over, the one named last changes fastest.
Arguments:
- factor_blocks: float32 [32, 32, 3, 256, 256], P('sub', 'row'), may hold values from -0.25 to 0.25
- block_inverses: float32 [32, 32, 256, 256], P('sub', 'row'), as said below
- band_offsets: int32 [32, 32, 3], P('sub', 'row'), may hold values from 1 to 4, as said below
- coupling: float32 [32, 8192, 512], P('sub', 'row'), may hold values from -0.0625 to 0.0625
- interface_block: float32 [32, 4, 128, 512], P('sub', None, 'row'), may hold values from -6 to 6
- tile_ids: int32 [32, 4], replicated, may hold values from 0 to 255, as said below
Outputs:
- schur_tiles: float32 [32, 4, 128, 512], P('sub', None, 'row')
The draws below stay inside these ranges and needn't reach their ends.
Inputs may be any that keep to these rules, and one draw needn't show every extreme that they name: `band_offsets`: each entry is one of the numbers 1 .. 4, the 3 entries of a block row are distinct and rising. `tile_ids`: A subdomain's 4 numbers are distinct; a number appears in at most two subdomains, and then in neighbouring ones (s and s + 1); every subdomain but the last shares one or two numbers with the next. `block_inverses`: each block is lower triangular with a diagonal between 0.5 and 1.
All inputs are finite; a program needn't handle non-finite values.
Results may differ from the reference program's by a relative error of at most 0.0003.
Values sent between devices are 32-bit elements; how exact they have to be, the bound alone decides.
A program may use at most 64 MiB of HBM per device.

```python
import jax
import jax.numpy as jnp
from jax import lax

BLK = 256
K = 3
P_SIZE = 512
TILE = 128
TILES = 4
NB = 32
NI = 8192
SUBS = 32


def draw_block_inverses(key, part):
    key_diag, key_low = jax.random.split(jax.random.fold_in(key, 11))
    shape = (SUBS, NB, BLK, BLK)
    diagonal = jnp.exp(jax.random.uniform(key_diag, (SUBS, NB, BLK), jnp.float32, jnp.log(0.5), 0.0))
    lower = jax.random.normal(key_low, shape, jnp.float32) * (0.5 / BLK ** 0.5)
    strict = jnp.tril(lower, -1)
    return strict + jnp.eye(BLK, dtype=jnp.float32) * diagonal[..., None]


def draw_band_offsets(key, part):
    excluded = jax.random.randint(jax.random.fold_in(key, 23), (SUBS, NB), 1, K + 2)
    base = jnp.arange(1, K + 1, dtype=jnp.int32)
    return (base + (base >= excluded[..., None]).astype(jnp.int32)).astype(jnp.int32)


def draw_tile_ids(key, part):
    key_share, key_order = jax.random.split(jax.random.fold_in(key, 37))
    positions = jnp.arange(SUBS, dtype=jnp.int32)
    shared = jax.random.randint(key_share, (SUBS,), 1, 3)
    shared = jnp.where(positions == SUBS - 1, 0, shared)
    left = jnp.concatenate([jnp.zeros((1,), jnp.int32), shared[:-1]])
    slots = jnp.arange(TILES, dtype=jnp.int32)[None, :]
    owner = positions[:, None]
    left_id = 2 * TILES * (owner - 1) + TILES + slots
    private_id = 2 * TILES * owner + (slots - left[:, None])
    right_id = 2 * TILES * owner + TILES + (slots - (TILES - shared[:, None]))
    ordered = jnp.where(slots < left[:, None], left_id, jnp.where(slots < TILES - shared[:, None], private_id, right_id))
    scores = jax.random.randint(key_order, (SUBS, TILES), 0, 2 ** 20) * TILES + slots
    order = jnp.argsort(scores, axis=1)
    return jnp.take_along_axis(ordered, order, axis=1).astype(jnp.int32)


def shard_levels(stream_key, shape, cuts, least, top_value):
    gain = 1.0
    for axis_at, blocks in cuts:
        steps = jax.random.uniform(jax.random.fold_in(jax.random.fold_in(stream_key, 6), axis_at), (blocks,), jnp.float32, least / len(cuts), top_value / len(cuts))
        gain = gain * jnp.repeat(jnp.exp(steps), shape[axis_at] // blocks).reshape((-1,) + (1,) * (len(shape) - 1 - axis_at))
    return gain


def gaussian(rng, extent, scale, bound, cuts=(), kind=jnp.bfloat16):
    drawn = scale * jax.random.normal(rng, extent, jnp.float32)
    if cuts:
        drawn = drawn * shard_levels(rng, extent, cuts, -0.22, 0.18)
    return jnp.clip(drawn, -bound, bound).astype(kind)


def setup_inputs(seed: int = 0) -> dict:
    splits = jax.random.split(jax.random.key(seed), 7)
    return {
        "factor_blocks": gaussian(splits[0], (SUBS, NB, K, BLK, BLK), (5 * BLK // 2) ** -0.5, 0.25, ((0, 32), (1, 8)), jnp.float32),
        "block_inverses": draw_block_inverses(jax.random.fold_in(splits[6], 71), 0),
        "band_offsets": draw_band_offsets(jax.random.fold_in(splits[6], 71), 0),
        "coupling": gaussian(splits[3], (SUBS, NI, P_SIZE), NI ** -0.5, 0.0625, ((0, 32), (1, 8)), jnp.float32),
        "interface_block": gaussian(splits[4], (SUBS, TILES, TILE, P_SIZE), 1.0, 6.0, ((0, 32), (2, 8)), jnp.float32),
        "tile_ids": draw_tile_ids(jax.random.fold_in(splits[6], 71), 0),
    }


def solve_subdomain(blocks, inverses, offsets, coupling):
    right_side = coupling.reshape(NB, BLK, P_SIZE)
    padded = jnp.zeros((NB + K + 1, BLK, P_SIZE), jnp.float32)

    def substitute(row_block, padded):
        running = lax.dynamic_index_in_dim(right_side, row_block, 0, keepdims=False)
        factor_row = lax.dynamic_index_in_dim(blocks, row_block, 0, keepdims=False)
        offset_row = lax.dynamic_index_in_dim(offsets, row_block, 0, keepdims=False)
        for band in range(K):
            source_index = (row_block + K + 1 - offset_row[band]).astype(jnp.int32)
            source = lax.dynamic_index_in_dim(padded, source_index, 0, keepdims=False)
            running = running - jnp.dot(factor_row[band], source, precision=lax.Precision.HIGHEST)
        inverse = lax.dynamic_index_in_dim(inverses, row_block, 0, keepdims=False)
        solved_row = jnp.dot(inverse, running, precision=lax.Precision.HIGHEST)
        target = (row_block + K + 1).astype(jnp.int32)
        return lax.dynamic_update_index_in_dim(padded, solved_row, target, 0)

    padded = lax.fori_loop(jnp.int32(0), jnp.int32(NB), substitute, padded)
    flattened = padded[K + 1:].reshape(NI, P_SIZE)
    gram = lax.dot_general(flattened, flattened, (((0,), (0,)), ((), ())), precision=lax.Precision.HIGHEST)
    return gram.reshape(TILES, TILE, P_SIZE)


def reference(factor_blocks, block_inverses, band_offsets, coupling, interface_block, tile_ids):
    grams = lax.map(lambda args: solve_subdomain(*args), (factor_blocks, block_inverses, band_offsets, coupling))
    zero_gram = jnp.zeros((1, TILES, TILE, P_SIZE), jnp.float32)
    padded_grams = jnp.concatenate([zero_gram, grams, zero_gram], 0)
    positions = jnp.arange(SUBS, dtype=jnp.int32)
    contribution = jnp.zeros((SUBS, TILES, TILE, TILES, TILE), jnp.float32)
    for delta in range(3):
        neighbour_gram = padded_grams[delta:delta + SUBS].reshape(SUBS, TILES, TILE, TILES, TILE)
        neighbour_pos = jnp.clip(positions + delta - 1, 0, SUBS - 1).astype(jnp.int32)
        neighbour_ids = tile_ids[neighbour_pos]
        match = (tile_ids[:, :, None] == neighbour_ids[:, None, :]).astype(jnp.float32)
        contribution = contribution + jnp.einsum('sik,sjl,skalb->siajb', match, match, neighbour_gram, precision=lax.Precision.HIGHEST)
    return interface_block - contribution.reshape(SUBS, TILES, TILE, P_SIZE)
```

```python
import functools

import jax
import jax.numpy as jnp
from jax import lax
from jax.experimental import pallas as pl
from jax.experimental.pallas import tpu as pltpu
from jax.sharding import PartitionSpec as P

MESH = pl.DeviceIdType.MESH
F32 = jnp.float32
BF16 = jnp.bfloat16
CHUNK = 16
NT = (((1,), (1,)), ((), ()))
NN = (((1,), (0,)), ((), ()))


def split(value):
    high = value.astype(BF16)
    low = (value - high.astype(F32)).astype(BF16)
    return high, low


def dot(a, b, dims):
    return lax.dot_general(a, b, dims, preferred_element_type=F32)


def dot3(ah, al, bh, bl, dims=NT):
    return dot(ah, bh, dims) + dot(ah, bl, dims) + dot(al, bh, dims)


def kernel(
    subs,
    rows,
    factor,
    inverse,
    offsets,
    coupling,
    interface,
    tile_ids,
    out,
    lh,
    ll,
    ih,
    il,
    yt,
    yh,
    yl,
    wh,
    wl,
    arrived,
    gpart,
    grecv,
    gsum,
    nearby,
    chain_send,
    chain_recv,
    gram_send,
    gram_recv,
    near_send,
    near_recv,
):
    sub = lax.axis_index("sub")
    row = lax.axis_index("row")
    brows, kband, block, _ = factor.shape
    cols = coupling.shape[1]
    chunks = cols // CHUNK
    tiles, share, _ = interface.shape
    tile = cols // tiles

    nearby[...] = jnp.zeros_like(nearby)

    barrier = pltpu.get_barrier_semaphore()
    for step in range(1, rows):
        pl.semaphore_signal(
            barrier, inc=1, device_id=(sub, lax.rem(row + step, rows)), device_id_type=MESH
        )
    has_left = sub > 0
    has_right = sub < subs - 1

    @pl.when(has_left)
    def _():
        pl.semaphore_signal(barrier, inc=1, device_id=(sub - 1, row), device_id_type=MESH)

    @pl.when(has_right)
    def _():
        pl.semaphore_signal(barrier, inc=1, device_id=(sub + 1, row), device_id_type=MESH)

    for r in range(brows):
        for offset in range(1, brows + 1):
            value = jnp.zeros((block, block), F32)
            for band in range(kband):
                if band + 1 <= offset <= band + 2:
                    value = jnp.where(offsets[r, band] == offset, factor[r, band], value)
            high, low = split(value)
            lh[r * brows + offset - 1] = high
            ll[r * brows + offset - 1] = low
        high, low = split(inverse[r])
        ih[r] = high
        il[r] = low

    def span(r):
        return slice(r * block, (r + 1) * block)

    for r in range(brows):
        right = coupling[span(r), :].T
        for offset in range(1, r + 1):
            s = span(r - offset)
            i = r * brows + offset - 1
            right = right - dot3(yh[:, s], yl[:, s], lh[i], ll[i])
        high, low = split(right)
        solved = dot3(high, low, ih[r], il[r])
        yt[:, span(r)] = solved
        high, low = split(solved)
        yh[:, span(r)] = high
        yl[:, span(r)] = low

    pl.semaphore_wait(barrier, rows - 1 + has_left.astype(jnp.int32) + has_right.astype(jnp.int32))

    following = lax.rem(row + 1, rows)

    def rows_of(c):
        return pl.ds(pl.multiple_of(c * CHUNK, CHUNK), CHUNK)

    def chain_copy(c):
        return pltpu.make_async_remote_copy(
            src_ref=yt.at[rows_of(c)],
            dst_ref=arrived.at[rows_of(c)],
            send_sem=chain_send.at[c],
            recv_sem=chain_recv.at[c],
            device_id=(sub, following),
            device_id_type=MESH,
        )

    @pl.when(row == 0)
    def _():
        @pl.loop(0, chunks)
        def _(c):
            chain_copy(c).start()

    @pl.when(row > 0)
    def _():
        @pl.loop(0, brows)
        def _(b):
            k = pl.ds(pl.multiple_of(b * block, block), block)
            for r in range(brows):
                i = jnp.clip(r * brows + brows + r - b - 1, 0, brows * brows - 1)
                placed = lh[i].astype(F32) + ll[i].astype(F32)
                right = jnp.where(b >= r, -placed.T, 0.0)
                for offset in range(1, r + 1):
                    s = span(r - offset)
                    j = r * brows + offset - 1
                    right = right - dot3(wh[k, s], wl[k, s], lh[j], ll[j])
                high, low = split(right)
                solved = dot3(high, low, ih[r], il[r])
                high, low = split(solved)
                wh[k, span(r)] = high
                wl[k, span(r)] = low

        @pl.loop(0, chunks)
        def _(c):
            chain_copy(c).wait_recv()
            here = rows_of(c)
            high, low = split(arrived[here, :])
            both = dot(jnp.concatenate([high, low], 0), wh[...], NN)
            value = yt[here, :] + (both[:CHUNK] + (both[CHUNK:] + dot(high, wl[...], NN)))
            yt[here, :] = value

            @pl.when(row < rows - 1)
            def _():
                chain_copy(c).start()

            high, low = split(value)
            yh[here, :] = high
            yl[here, :] = low

    half = cols // 2
    for part in range(2):
        mine = pl.ds(part * half, half)
        gram = dot3(yh[mine, :], yl[mine, :], yh[...], yl[...])
        for k in range(half // tile):
            for r in range(rows):
                at = k * tile + r * share
                gpart[r, part * (half // tile) + k] = gram[at : at + share]

    def gram_copy(step):
        to = lax.rem(row + step, rows)
        return pltpu.make_async_remote_copy(
            src_ref=gpart.at[to],
            dst_ref=grecv.at[step],
            send_sem=gram_send.at[step],
            recv_sem=gram_recv.at[step],
            device_id=(sub, to),
            device_id_type=MESH,
        )

    for step in range(1, rows):
        gram_copy(step).start()
    total = gpart[row]
    for step in range(1, rows):
        gram_copy(step).wait_recv()
        total = total + grecv[step]
    gsum[...] = total

    def near_copy(side):
        return pltpu.make_async_remote_copy(
            src_ref=gsum,
            dst_ref=nearby.at[side],
            send_sem=near_send.at[side],
            recv_sem=near_recv.at[side],
            device_id=(sub + 1 if side == 0 else sub - 1, row),
            device_id_type=MESH,
        )

    @pl.when(has_right)
    def _():
        near_copy(0).start()

    @pl.when(has_left)
    def _():
        near_copy(1).start()

    left = jnp.maximum(sub - 1, 0)
    right = jnp.minimum(sub + 1, subs - 1)

    @pl.when(has_left)
    def _():
        near_copy(0).wait_recv()

    @pl.when(has_right)
    def _():
        near_copy(1).wait_recv()

    result = interface[...] - gsum[...]
    for side, (other, exists) in enumerate(((left, has_left), (right, has_right))):
        match = [
            [
                jnp.where((tile_ids[sub, i] == tile_ids[other, k]) & exists, 1.0, 0.0)
                for k in range(tiles)
            ]
            for i in range(tiles)
        ]
        gram = nearby[side]
        taken = []
        for i in range(tiles):
            across = sum(match[i][k] * gram[k] for k in range(tiles))
            pieces = [
                sum(match[j][m] * across[:, m * tile : (m + 1) * tile] for m in range(tiles))
                for j in range(tiles)
            ]
            taken.append(jnp.concatenate(pieces, 1))
        result = result - jnp.stack(taken)
    out[...] = result

    @pl.when(row < rows - 1)
    def _():
        @pl.loop(0, chunks)
        def _(c):
            chain_copy(c).wait_send()

    for step in range(1, rows):
        gram_copy(step).wait_send()

    @pl.when(has_right)
    def _():
        near_copy(0).wait_send()

    @pl.when(has_left)
    def _():
        near_copy(1).wait_send()


def shards(
    subs, rows, factor_blocks, block_inverses, band_offsets, coupling, interface_block, tile_ids
):
    brows, _, block, _ = factor_blocks.shape[1:]
    height, cols = coupling.shape[1:]
    tiles, share, _ = interface_block.shape[1:]
    vmem = pl.BlockSpec(memory_space=pltpu.VMEM)
    smem = pl.BlockSpec(memory_space=pltpu.SMEM)
    scratch = [
        pltpu.VMEM((brows * brows, block, block), BF16),
        pltpu.VMEM((brows * brows, block, block), BF16),
        pltpu.VMEM((brows, block, block), BF16),
        pltpu.VMEM((brows, block, block), BF16),
        pltpu.VMEM((cols, height), F32),
        pltpu.VMEM((cols, height), BF16),
        pltpu.VMEM((cols, height), BF16),
        pltpu.VMEM((height, height), BF16),
        pltpu.VMEM((height, height), BF16),
        pltpu.VMEM((cols, height), F32),
        pltpu.VMEM((rows, tiles, share, cols), F32),
        pltpu.VMEM((rows, tiles, share, cols), F32),
        pltpu.VMEM((tiles, share, cols), F32),
        pltpu.VMEM((2, tiles, share, cols), F32),
        pltpu.SemaphoreType.DMA((cols // CHUNK,)),
        pltpu.SemaphoreType.DMA((cols // CHUNK,)),
        pltpu.SemaphoreType.DMA((rows,)),
        pltpu.SemaphoreType.DMA((rows,)),
        pltpu.SemaphoreType.DMA((2,)),
        pltpu.SemaphoreType.DMA((2,)),
    ]
    result = pl.pallas_call(
        functools.partial(kernel, subs, rows),
        out_shape=jax.ShapeDtypeStruct((tiles, share, cols), F32),
        in_specs=[vmem, vmem, smem, vmem, vmem, smem],
        out_specs=vmem,
        scratch_shapes=scratch,
        compiler_params=pltpu.CompilerParams(
            collective_id=0, has_side_effects=True, vmem_limit_bytes=60 * 1024 * 1024
        ),
    )(
        factor_blocks[0],
        block_inverses[0],
        band_offsets[0],
        coupling[0],
        interface_block[0],
        tile_ids,
    )
    return result[None]


def solution(mesh):
    return jax.shard_map(
        functools.partial(shards, mesh.shape["sub"], mesh.shape["row"]),
        mesh=mesh,
        in_specs=(
            P("sub", "row", None, None, None),
            P("sub", "row", None, None),
            P("sub", "row", None),
            P("sub", "row", None),
            P("sub", None, "row", None),
            P(),
        ),
        out_specs=P("sub", None, "row", None),
        check_vma=False,
    )
```

```python
import functools

import jax
import jax.numpy as jnp
from jax import lax
from jax.experimental import pallas as pl
from jax.experimental.pallas import tpu as pltpu
from jax.sharding import PartitionSpec as P

MESH = pl.DeviceIdType.MESH
F32 = jnp.float32
BF16 = jnp.bfloat16
CHUNK = 16
NT = (((1,), (1,)), ((), ()))
NN = (((1,), (0,)), ((), ()))


def split(value):
    high = value.astype(BF16)
    low = (value - high.astype(F32)).astype(BF16)
    return high, low


def dot(a, b, dims):
    return lax.dot_general(a, b, dims, preferred_element_type=F32)


def dot3(ah, al, bh, bl, dims=NT):
    return dot(ah, bh, dims) + dot(ah, bl, dims) + dot(al, bh, dims)


def kernel(
    subs,
    rows,
    factor_hbm,
    inverse_hbm,
    offsets,
    coupling_hbm,
    tile_ids,
    out,
    factor,
    inverse,
    coupling,
    nh,
    nl,
    ih,
    il,
    yt,
    yh,
    yl,
    wh,
    wl,
    arrived,
    gpart,
    grecv,
    gsum,
    nearby,
    load_sem,
    chain_send,
    chain_recv,
    gram_send,
    gram_recv,
    near_send,
    near_recv,
):
    sub = lax.axis_index("sub")
    row = lax.axis_index("row")
    brows, kband, block, _ = factor.shape
    height, cols = coupling.shape
    chunks = cols // CHUNK
    tiles = tile_ids.shape[0]
    tile = cols // tiles
    share = tile // rows
    odd = lax.rem(row, 2) == 1
    last = row == rows - 1

    loads = [
        pltpu.make_async_copy(source, target, load_sem.at[i])
        for i, (source, target) in enumerate(
            ((inverse_hbm, inverse), (factor_hbm, factor), (coupling_hbm, coupling))
        )
    ]
    for load in loads:
        load.start()

    nearby[...] = jnp.zeros_like(nearby)

    barrier = pltpu.get_barrier_semaphore()
    for step in range(1, rows):
        pl.semaphore_signal(
            barrier, inc=1, device_id=(sub, lax.rem(row + step, rows)), device_id_type=MESH
        )
    has_left = sub > 0
    has_right = sub < subs - 1

    @pl.when(has_left)
    def _():
        pl.semaphore_signal(barrier, inc=1, device_id=(sub - 1, row), device_id_type=MESH)

    @pl.when(has_right)
    def _():
        pl.semaphore_signal(barrier, inc=1, device_id=(sub + 1, row), device_id_type=MESH)

    def span(r):
        return slice(r * block, (r + 1) * block)

    def own(r):
        return slice(height + r * block, height + (r + 1) * block)

    def at_offset(r, offset):
        value = jnp.zeros((block, block), F32)
        for band in range(kband):
            if band + 1 <= offset <= band + 2:
                value = jnp.where(offsets[band, 0, r] == offset, factor[r, band], value)
        return value

    def local(r, offset):
        return r * (r - 1) // 2 + offset - 1

    loads[0].wait()
    for r in range(brows):
        high, low = split(inverse[r])
        ih[r] = high
        il[r] = low
    loads[1].wait()
    for r in range(1, brows):
        for offset in range(1, r + 1):
            high, low = split(at_offset(r, offset))
            high, low = split(dot3(ih[r], il[r], high, low, NN))
            nh[local(r, offset)] = high
            nl[local(r, offset)] = low

    loads[2].wait()
    for r in range(brows):
        high, low = split(coupling[span(r), :].T)
        solved = dot3(high, low, ih[r], il[r])
        for offset in range(r, 0, -1):
            s = own(r - offset)
            n = local(r, offset)
            solved = solved - dot3(yh[:, s], yl[:, s], nh[n], nl[n])
        yt[:, span(r)] = solved
        high, low = split(solved)
        yh[:, own(r)] = high
        yl[:, own(r)] = low

    pl.semaphore_wait(
        barrier, rows - 1 + has_left.astype(jnp.int32) + has_right.astype(jnp.int32)
    )

    following = lax.rem(row + 1, rows)

    def rows_of(c):
        return pl.ds(pl.multiple_of(c * CHUNK, CHUNK), CHUNK)

    def chain_copy(c):
        return pltpu.make_async_remote_copy(
            src_ref=yt.at[rows_of(c)],
            dst_ref=arrived.at[rows_of(c)],
            send_sem=chain_send.at[c],
            recv_sem=chain_recv.at[c],
            device_id=(sub, following),
            device_id_type=MESH,
        )

    def stage(q):
        return pl.ds(q * q, 2 * q + 1)

    def gram_copy(q, step):
        to = lax.rem(row + step, rows)
        return pltpu.make_async_remote_copy(
            src_ref=gpart.at[to, stage(q)],
            dst_ref=grecv.at[row // 2, stage(q)],
            send_sem=gram_send.at[q, step],
            recv_sem=gram_recv.at[q, row // 2],
            device_id=(sub, to),
            device_id_type=MESH,
        )

    def gram_stage(q):
        mine = slice(q * tile, (q + 1) * tile)
        upto = slice(0, (q + 1) * tile)
        high = yh[mine, :]
        both = dot(jnp.concatenate([high, yl[mine, :]], 0), yh[upto, :], NT)
        gram = both[:tile] + (both[tile:] + dot(high, yl[upto, :], NT))
        for l in range(q + 1):
            part = gram[:, l * tile : (l + 1) * tile]
            gpart[:, q * q + l] = part.reshape(rows, share, tile)
            if l < q:
                gpart[:, q * q + q + 1 + l] = part.T.reshape(rows, share, tile)
        for step in range(1, rows):
            gram_copy(q, step).start()
        grecv[row // 2, stage(q)] = gpart[row, stage(q)]

    @pl.when(row == 0)
    def _():
        @pl.loop(0, chunks)
        def _(c):
            chain_copy(c).start()

    @pl.when(row > 0)
    def _():
        for b in range(brows):
            for r in range(b + 1):
                high, low = split(-at_offset(r, brows + r - b).T)
                wh[span(b), span(r)] = high
                wl[span(b), span(r)] = low
        for b0 in range(0, brows, 2):
            k = slice(b0 * block, (b0 + 2) * block)
            for r in range(brows):
                solved = None
                first = max(r, b0)
                if first < b0 + 2:
                    part = slice(first * block, (b0 + 2) * block)
                    solved = dot3(wh[part, span(r)], wl[part, span(r)], ih[r], il[r])
                    if first > b0:
                        solved = jnp.concatenate(
                            [jnp.zeros(((first - b0) * block, block), F32), solved], 0
                        )
                for offset in range(r, 0, -1):
                    s = span(r - offset)
                    n = local(r, offset)
                    term = dot3(wh[k, s], wl[k, s], nh[n], nl[n])
                    solved = -term if solved is None else solved - term
                high, low = split(solved)
                wh[k, span(r)] = high
                wl[k, span(r)] = low

        @pl.loop(0, chunks)
        def _(c):
            chain_copy(c).wait_recv()
            here = rows_of(c)
            high, low = split(arrived[here, :])
            both = dot(jnp.concatenate([high, low], 0), wh[...], NN)
            value = yt[here, :] + (both[:CHUNK] + (both[CHUNK:] + dot(high, wl[...], NN)))
            yt[here, :] = value

            @pl.when(row < rows - 1)
            def _():
                chain_copy(c).start()

            yh[here, :height] = high
            yl[here, :height] = low
            high, low = split(value)
            yh[here, height:] = high
            yl[here, height:] = low

            for q in range(tiles - 1):
                @pl.when(last & (c == (q + 1) * (chunks // tiles) - 1))
                def _():
                    gram_stage(q)

    @pl.when(odd & (row < rows - 1))
    def _():
        for q in range(tiles - 1):
            gram_stage(q)

    @pl.when(odd)
    def _():
        gram_stage(tiles - 1)

    def near_copy(side, q):
        return pltpu.make_async_remote_copy(
            src_ref=gsum.at[stage(q)],
            dst_ref=nearby.at[side, stage(q)],
            send_sem=near_send.at[side, q],
            recv_sem=near_recv.at[side, q],
            device_id=(sub + 1 if side == 0 else sub - 1, row),
            device_id_type=MESH,
        )

    for q in range(tiles):
        for j in range(rows // 2):
            @pl.when(row != 2 * j + 1)
            def _():
                pltpu.make_async_remote_copy(
                    src_ref=gpart.at[0, stage(q)],
                    dst_ref=grecv.at[j, stage(q)],
                    send_sem=gram_send.at[q, 0],
                    recv_sem=gram_recv.at[q, j],
                    device_id=(sub, following),
                    device_id_type=MESH,
                ).wait_recv()
        total = grecv[0, stage(q)]
        for j in range(1, rows // 2):
            total = total + grecv[j, stage(q)]
        gsum[stage(q)] = total

        @pl.when(has_right)
        def _():
            near_copy(0, q).start()

        @pl.when(has_left)
        def _():
            near_copy(1, q).start()

    for q in range(tiles):
        @pl.when(has_left)
        def _():
            near_copy(0, q).wait_recv()

        @pl.when(has_right)
        def _():
            near_copy(1, q).wait_recv()

    def index(k, l):
        return k * k + l if k >= l else l * l + l + 1 + k

    left = jnp.maximum(sub - 1, 0)
    right = jnp.minimum(sub + 1, subs - 1)
    matches = [
        [
            [
                jnp.where((tile_ids[i, sub] == tile_ids[k, other]) & exists, 1.0, 0.0)
                for k in range(tiles)
            ]
            for i in range(tiles)
        ]
        for other, exists in ((left, has_left), (right, has_right))
    ]
    for i in range(tiles):
        across = [
            [sum(match[i][k] * nearby[side, index(k, m)] for k in range(tiles)) for m in range(tiles)]
            for side, match in enumerate(matches)
        ]
        for j in range(tiles):
            value = gsum[index(i, j)]
            for match, taken in zip(matches, across):
                value = value + sum(match[j][m] * taken[m] for m in range(tiles))
            out[i, :, j * tile : (j + 1) * tile] = value

    @pl.when(row < rows - 1)
    def _():
        @pl.loop(0, chunks)
        def _(c):
            chain_copy(c).wait_send()

    @pl.when(odd)
    def _():
        for q in range(tiles):
            for step in range(1, rows):
                gram_copy(q, step).wait_send()

    for q in range(tiles):
        @pl.when(has_right)
        def _():
            near_copy(0, q).wait_send()

        @pl.when(has_left)
        def _():
            near_copy(1, q).wait_send()


def shards(
    subs, rows, factor_blocks, block_inverses, band_offsets, coupling, interface_block, tile_ids
):
    brows, kband, block, _ = factor_blocks.shape[1:]
    height, cols = coupling.shape[1:]
    tiles, share, _ = interface_block.shape[1:]
    tile = cols // tiles
    locals_ = brows * (brows - 1) // 2
    hbm = pl.BlockSpec(memory_space=pl.ANY)
    vmem = pl.BlockSpec(memory_space=pltpu.VMEM)
    smem = pl.BlockSpec(memory_space=pltpu.SMEM)
    dma = pltpu.SemaphoreType.DMA
    scratch = [
        pltpu.VMEM((brows, kband, block, block), F32),
        pltpu.VMEM((brows, block, block), F32),
        pltpu.VMEM((height, cols), F32),
        pltpu.VMEM((locals_, block, block), BF16),
        pltpu.VMEM((locals_, block, block), BF16),
        pltpu.VMEM((brows, block, block), BF16),
        pltpu.VMEM((brows, block, block), BF16),
        pltpu.VMEM((cols, height), F32),
        pltpu.VMEM((cols, 2 * height), BF16),
        pltpu.VMEM((cols, 2 * height), BF16),
        pltpu.VMEM((height, height), BF16),
        pltpu.VMEM((height, height), BF16),
        pltpu.VMEM((cols, height), F32),
        pltpu.VMEM((rows, tiles * tiles, share, tile), F32),
        pltpu.VMEM((rows // 2, tiles * tiles, share, tile), F32),
        pltpu.VMEM((tiles * tiles, share, tile), F32),
        pltpu.VMEM((2, tiles * tiles, share, tile), F32),
        dma((3,)),
        dma((cols // CHUNK,)),
        dma((cols // CHUNK,)),
        dma((tiles, rows)),
        dma((tiles, rows // 2)),
        dma((2, tiles)),
        dma((2, tiles)),
    ]
    contribution = pl.pallas_call(
        functools.partial(kernel, subs, rows),
        out_shape=jax.ShapeDtypeStruct((tiles, share, cols), F32),
        in_specs=[hbm, hbm, smem, hbm, smem],
        out_specs=vmem,
        scratch_shapes=scratch,
        compiler_params=pltpu.CompilerParams(
            collective_id=0, has_side_effects=True, vmem_limit_bytes=60 * 1024 * 1024
        ),
    )(
        factor_blocks[0],
        block_inverses[0],
        jnp.transpose(band_offsets, (2, 0, 1)),
        coupling[0],
        tile_ids.T,
    )
    return interface_block - contribution[None]


def solution(mesh):
    return jax.shard_map(
        functools.partial(shards, mesh.shape["sub"], mesh.shape["row"]),
        mesh=mesh,
        in_specs=(
            P("sub", "row", None, None, None),
            P("sub", "row", None, None),
            P("sub", "row", None),
            P("sub", "row", None),
            P("sub", None, "row", None),
            P(),
        ),
        out_specs=P("sub", None, "row", None),
        check_vma=False,
    )
```

```python
import functools

import jax
import jax.numpy as jnp
from jax import lax
from jax.experimental import pallas as pl
from jax.experimental.pallas import tpu as pltpu
from jax.sharding import PartitionSpec as P

MESH = pl.DeviceIdType.MESH
F32 = jnp.float32
BF16 = jnp.bfloat16
CHUNK = 16
NT = (((1,), (1,)), ((), ()))
NN = (((1,), (0,)), ((), ()))


def split(value):
    high = value.astype(BF16)
    low = (value - high.astype(F32)).astype(BF16)
    return high, low


def dot(a, b, dims):
    return lax.dot_general(a, b, dims, preferred_element_type=F32)


def dot3(ah, al, bh, bl, dims=NT):
    return dot(ah, bh, dims) + dot(ah, bl, dims) + dot(al, bh, dims)


def kernel(
    subs,
    rows,
    factor_hbm,
    inverse_hbm,
    offsets,
    coupling_hbm,
    tile_ids,
    out,
    factor,
    inverse,
    coupling,
    nh,
    nl,
    ih,
    il,
    yt,
    yh,
    yl,
    wh,
    wl,
    arrived,
    gpart,
    grecv,
    gsum,
    perm,
    shared,
    nearby,
    load_sem,
    chain_send,
    chain_recv,
    gram_send,
    gram_recv,
    stage_send,
    stage_recv,
    near_send,
    near_recv,
    go,
):
    sub = lax.axis_index("sub")
    row = lax.axis_index("row")
    brows, kband, block, _ = factor.shape
    height, cols = coupling.shape
    chunks = cols // CHUNK
    tiles = tile_ids.shape[0]
    tile = cols // tiles
    share = tile // rows
    half = rows // 2
    parity = lax.rem(row, 2)
    odd = parity == 1
    mine = row // 2
    piece = tiles * share
    lanes = 2 * piece
    parts = cols // lanes
    last = row == rows - 1

    loads = [
        pltpu.make_async_copy(source, target, load_sem.at[i])
        for i, (source, target) in enumerate(
            ((inverse_hbm, inverse), (factor_hbm, factor), (coupling_hbm, coupling))
        )
    ]
    for load in loads:
        load.start()

    nearby[...] = jnp.zeros_like(nearby)

    barrier = pltpu.get_barrier_semaphore()
    for step in range(1, rows):
        pl.semaphore_signal(
            barrier, inc=1, device_id=(sub, lax.rem(row + step, rows)), device_id_type=MESH
        )
    has_left = sub > 0
    has_right = sub < subs - 1

    @pl.when(has_left)
    def _():
        pl.semaphore_signal(barrier, inc=1, device_id=(sub - 1, row), device_id_type=MESH)

    @pl.when(has_right)
    def _():
        pl.semaphore_signal(barrier, inc=1, device_id=(sub + 1, row), device_id_type=MESH)

    def span(r):
        return slice(r * block, (r + 1) * block)

    def own(r):
        return slice(height + r * block, height + (r + 1) * block)

    def at_offset(r, offset):
        value = jnp.zeros((block, block), F32)
        for band in range(kband):
            if band + 1 <= offset <= band + 2:
                value = jnp.where(offsets[band, 0, r] == offset, factor[r, band], value)
        return value

    def local(r, offset):
        return r * (r - 1) // 2 + offset - 1

    loads[0].wait()
    for r in range(brows):
        high, low = split(inverse[r])
        ih[r] = high
        il[r] = low
    loads[1].wait()
    for r in range(1, brows):
        for offset in range(1, r + 1):
            high, low = split(at_offset(r, offset))
            high, low = split(dot3(ih[r], il[r], high, low, NN))
            nh[local(r, offset)] = high
            nl[local(r, offset)] = low

    loads[2].wait()
    for r in range(brows):
        natural = coupling[span(r), :].T
        order = [
            k * tile + (2 * j + p) * share for p in range(2) for j in range(half) for k in range(tiles)
        ]
        high, low = split(jnp.concatenate([natural[n : n + share] for n in order], 0))
        solved = dot3(high, low, ih[r], il[r])
        for offset in range(r, 0, -1):
            s = own(r - offset)
            n = local(r, offset)
            solved = solved - dot3(yh[:, s], yl[:, s], nh[n], nl[n])
        yt[:, span(r)] = solved
        high, low = split(solved)
        yh[:, own(r)] = high
        yl[:, own(r)] = low

    pl.semaphore_wait(
        barrier, rows - 1 + has_left.astype(jnp.int32) + has_right.astype(jnp.int32)
    )

    following = lax.rem(row + 1, rows)

    def rows_of(c):
        return pl.ds(pl.multiple_of(c * CHUNK, CHUNK), CHUNK)

    def chain_copy(c):
        return pltpu.make_async_remote_copy(
            src_ref=yt.at[rows_of(c)],
            dst_ref=arrived.at[rows_of(c)],
            send_sem=chain_send.at[c],
            recv_sem=chain_recv.at[c],
            device_id=(sub, following),
            device_id_type=MESH,
        )

    def gram_of(start, count, part, width, depth):
        high = yh[start : start + count, depth:]
        low = yl[start : start + count, depth:]
        at = slice(part * lanes, part * lanes + width)
        both = dot(jnp.concatenate([high, low], 0), yh[at, depth:], NT)
        return both[:count] + (both[count:] + dot(high, yl[at, depth:], NT))

    def keep(gram, slot, part):
        for j in range(gram.shape[0] // piece):
            for m in range(gram.shape[1] // lanes):
                gpart[slot + j, part + m] = gram[
                    j * piece : (j + 1) * piece, m * lanes : (m + 1) * lanes
                ]

    def gram_copy(step):
        to = lax.rem(mine + step, half)
        return pltpu.make_async_remote_copy(
            src_ref=gpart.at[to],
            dst_ref=grecv.at[mine],
            send_sem=gram_send.at[step],
            recv_sem=gram_recv.at[mine],
            device_id=(sub, 2 * to + parity),
            device_id_type=MESH,
        )

    def stage_copy(q, j):
        even = j % 2 == 0
        if even:
            at = pl.ds(0, 2) if q == 1 else pl.ds(q, 1)
        else:
            first = (half + j // 2) // 2
            at = pl.ds(0, q + 1) if q == first else pl.ds(q, 1)
        return pltpu.make_async_remote_copy(
            src_ref=gpart.at[j // 2 + (half if even else 0), at],
            dst_ref=grecv.at[half if even else half - 1, at],
            send_sem=stage_send.at[q, j],
            recv_sem=stage_recv.at[q],
            device_id=(sub, j),
            device_id_type=MESH,
        )

    def targets(q):
        evens = [] if q == 0 else list(range(0, rows, 2))
        odds = [j for j in range(1, rows - 1, 2) if (half + j // 2) // 2 <= q]
        return odds + evens

    def gram_stage(q):
        own_rows = half * piece
        if q == 1:
            keep(gram_of(0, own_rows, 0, 2 * lanes, height), half, 0)
        if q >= 2:
            keep(gram_of(0, own_rows, q, lanes, height), half, q)
        if q == 2:
            keep(gram_of(own_rows, lanes, 0, (q + 1) * lanes, 0), 0, 0)
        if q == 3:
            keep(gram_of(own_rows, lanes, q, lanes, 0), 0, q)
            keep(gram_of(own_rows + lanes, lanes, 0, cols, 0), 2, 0)
        for j in targets(q):
            stage_copy(q, j).start()

    @pl.when(row == 0)
    def _():
        @pl.loop(0, chunks)
        def _(c):
            chain_copy(c).start()

        yh[:, :height] = jnp.zeros((cols, height), BF16)
        yl[:, :height] = jnp.zeros((cols, height), BF16)

    @pl.when(row > 0)
    def _():
        for b in range(brows):
            for r in range(b + 1):
                high, low = split(-at_offset(r, brows + r - b).T)
                wh[span(b), span(r)] = high
                wl[span(b), span(r)] = low
        for b0 in range(0, brows, 2):
            k = slice(b0 * block, (b0 + 2) * block)
            for r in range(brows):
                solved = None
                first = max(r, b0)
                if first < b0 + 2:
                    part = slice(first * block, (b0 + 2) * block)
                    solved = dot3(wh[part, span(r)], wl[part, span(r)], ih[r], il[r])
                    if first > b0:
                        solved = jnp.concatenate(
                            [jnp.zeros(((first - b0) * block, block), F32), solved], 0
                        )
                for offset in range(r, 0, -1):
                    s = span(r - offset)
                    n = local(r, offset)
                    term = dot3(wh[k, s], wl[k, s], nh[n], nl[n])
                    solved = -term if solved is None else solved - term
                high, low = split(solved)
                wh[k, span(r)] = high
                wl[k, span(r)] = low

        @pl.loop(0, chunks)
        def _(c):
            chain_copy(c).wait_recv()
            here = rows_of(c)
            high, low = split(arrived[here, :])
            both = dot(jnp.concatenate([high, low], 0), wh[...], NN)
            value = yt[here, :] + (both[:CHUNK] + (both[CHUNK:] + dot(high, wl[...], NN)))
            yt[here, :] = value

            @pl.when(row < rows - 1)
            def _():
                chain_copy(c).start()

            yh[here, :height] = high
            yl[here, :height] = low
            high, low = split(value)
            yh[here, height:] = high
            yl[here, height:] = low

            for q in range(1, parts - 1):
                @pl.when(last & (c == (q + 1) * (chunks // parts) - 1))
                def _():
                    gram_stage(q)

    @pl.when(last)
    def _():
        gram_stage(parts - 1)

    @pl.when(row < rows - 1)
    def _():
        @pl.when(odd)
        def _():
            keep(gram_of(half * piece, half * piece, 0, cols, 0), 0, 0)

        @pl.when(parity == 0)
        def _():
            keep(gram_of(0, half * piece, 0, cols, 0), 0, 0)

        @pl.when(row >= rows - 3)
        def _():
            for j in range(half - 1):
                @pl.when(2 * j + parity < rows - 3)
                def _():
                    pl.semaphore_signal(
                        go, inc=1, device_id=(sub, 2 * j + parity), device_id_type=MESH
                    )

        @pl.when(row < rows - 3)
        def _():
            pl.semaphore_wait(go, 1)

        for step in range(1, half):
            gram_copy(step).start()

    at_row = lax.broadcasted_iota(jnp.int32, (cols, cols), 0)
    at_col = lax.broadcasted_iota(jnp.int32, (cols, cols), 1)
    place = at_row // piece
    home = (
        (at_row % piece) // share * tile
        + (2 * (place % half) + place // half) * share
        + at_row % share
    )
    perm[...] = jnp.where(home == at_col, 1.0, 0.0).astype(BF16)

    grecv[mine] = gpart[mine]

    def arrival(sem, slot, at):
        return pltpu.make_async_remote_copy(
            src_ref=gpart.at[0, at],
            dst_ref=grecv.at[slot, at],
            send_sem=gram_send.at[0],
            recv_sem=sem,
            device_id=(sub, following),
            device_id_type=MESH,
        )

    everything = pl.ds(0, parts)
    for j in range(half):
        @pl.when((j != mine) & ((j < half - 1) | (parity == 0)))
        def _():
            arrival(gram_recv.at[j], j, everything).wait_recv()

    @pl.when(parity == 0)
    def _():
        arrival(stage_recv.at[1], half, pl.ds(0, 2)).wait_recv()
        arrival(stage_recv.at[2], half, pl.ds(2, 1)).wait_recv()
        arrival(stage_recv.at[3], half, pl.ds(3, 1)).wait_recv()

    @pl.when(odd & (row < rows - 3))
    def _():
        arrival(stage_recv.at[2], half - 1, pl.ds(0, 3)).wait_recv()
        arrival(stage_recv.at[3], half - 1, pl.ds(3, 1)).wait_recv()

    @pl.when(odd & (row == rows - 3))
    def _():
        arrival(stage_recv.at[3], half - 1, everything).wait_recv()

    total = []
    for m in range(parts):
        value = grecv[0, m]
        for j in range(1, half):
            value = value + grecv[j, m]
        total.append(value + jnp.where(odd, 0.0, grecv[half, m]))
    total = jnp.concatenate(total, 1)
    high = total.astype(BF16)
    rest = total - high.astype(F32)
    middle, low = split(rest)
    moved = dot(jnp.concatenate([high, middle, low], 0), perm[...], NN)
    moved = moved[:piece] + (moved[piece : 2 * piece] + moved[2 * piece :])
    for k in range(tiles):
        for l in range(tiles):
            gsum[k * tiles + l] = moved[k * share : (k + 1) * share, l * tile : (l + 1) * tile]

    def common(owner, other):
        first = jnp.int32(tiles - 1)
        second = jnp.int32(0)
        for k in range(tiles - 1, -1, -1):
            number = tile_ids[k, owner]
            hit = number == tile_ids[0, other]
            for m in range(1, tiles):
                hit = hit | (number == tile_ids[m, other])
            first = jnp.where(hit, k, first)
        for k in range(tiles):
            number = tile_ids[k, owner]
            hit = number == tile_ids[0, other]
            for m in range(1, tiles):
                hit = hit | (number == tile_ids[m, other])
            second = jnp.where(hit, k, second)
        return first, second

    left = jnp.maximum(sub - 1, 0)
    right = jnp.minimum(sub + 1, subs - 1)

    def near_copy(side):
        return pltpu.make_async_remote_copy(
            src_ref=shared.at[side],
            dst_ref=nearby.at[side],
            send_sem=near_send.at[side],
            recv_sem=near_recv.at[side],
            device_id=(sub + 1 if side == 0 else sub - 1, row),
            device_id_type=MESH,
        )

    for side, (other, exists) in enumerate(((right, has_right), (left, has_left))):
        pair = common(sub, other)
        for p in range(2):
            for m in range(2):
                shared[side, 2 * p + m] = gsum[pair[p] * tiles + pair[m]]

        @pl.when(exists)
        def _():
            near_copy(side).start()

    matches = []
    for other, exists in ((left, has_left), (right, has_right)):
        first, second = common(other, sub)
        matches.append(
            [
                [
                    jnp.where((tile_ids[i, sub] == tile_ids[first, other]) & exists, 1.0, 0.0)
                    for i in range(tiles)
                ],
                [
                    jnp.where(
                        (tile_ids[i, sub] == tile_ids[second, other])
                        & exists
                        & (first != second),
                        1.0,
                        0.0,
                    )
                    for i in range(tiles)
                ],
            ]
        )

    @pl.when(has_left)
    def _():
        near_copy(0).wait_recv()

    @pl.when(has_right)
    def _():
        near_copy(1).wait_recv()

    for i in range(tiles):
        across = [
            [match[0][i] * nearby[side, m] + match[1][i] * nearby[side, 2 + m] for m in range(2)]
            for side, match in enumerate(matches)
        ]
        for j in range(tiles):
            value = gsum[i * tiles + j]
            for match, taken in zip(matches, across):
                value = value + (match[0][j] * taken[0] + match[1][j] * taken[1])
            out[i, :, j * tile : (j + 1) * tile] = value

    @pl.when(row < rows - 1)
    def _():
        @pl.loop(0, chunks)
        def _(c):
            chain_copy(c).wait_send()

        for step in range(1, half):
            gram_copy(step).wait_send()

    @pl.when(last)
    def _():
        for q in range(1, parts):
            for j in targets(q):
                stage_copy(q, j).wait_send()

    @pl.when(has_right)
    def _():
        near_copy(0).wait_send()

    @pl.when(has_left)
    def _():
        near_copy(1).wait_send()


def shards(
    subs, rows, factor_blocks, block_inverses, band_offsets, coupling, interface_block, tile_ids
):
    brows, kband, block, _ = factor_blocks.shape[1:]
    height, cols = coupling.shape[1:]
    tiles, share, _ = interface_block.shape[1:]
    tile = cols // tiles
    piece = tiles * share
    lanes = 2 * piece
    parts = cols // lanes
    locals_ = brows * (brows - 1) // 2
    hbm = pl.BlockSpec(memory_space=pl.ANY)
    vmem = pl.BlockSpec(memory_space=pltpu.VMEM)
    smem = pl.BlockSpec(memory_space=pltpu.SMEM)
    dma = pltpu.SemaphoreType.DMA
    scratch = [
        pltpu.VMEM((brows, kband, block, block), F32),
        pltpu.VMEM((brows, block, block), F32),
        pltpu.VMEM((height, cols), F32),
        pltpu.VMEM((locals_, block, block), BF16),
        pltpu.VMEM((locals_, block, block), BF16),
        pltpu.VMEM((brows, block, block), BF16),
        pltpu.VMEM((brows, block, block), BF16),
        pltpu.VMEM((cols, height), F32),
        pltpu.VMEM((cols, 2 * height), BF16),
        pltpu.VMEM((cols, 2 * height), BF16),
        pltpu.VMEM((height, height), BF16),
        pltpu.VMEM((height, height), BF16),
        pltpu.VMEM((cols, height), F32),
        pltpu.VMEM((rows, parts, piece, lanes), F32),
        pltpu.VMEM((rows // 2 + 1, parts, piece, lanes), F32),
        pltpu.VMEM((tiles * tiles, share, tile), F32),
        pltpu.VMEM((cols, cols), BF16),
        pltpu.VMEM((2, 4, share, tile), F32),
        pltpu.VMEM((2, 4, share, tile), F32),
        dma((3,)),
        dma((cols // CHUNK,)),
        dma((cols // CHUNK,)),
        dma((rows // 2,)),
        dma((rows // 2,)),
        dma((parts, rows)),
        dma((parts,)),
        dma((2,)),
        dma((2,)),
        pltpu.SemaphoreType.REGULAR,
    ]
    contribution = pl.pallas_call(
        functools.partial(kernel, subs, rows),
        out_shape=jax.ShapeDtypeStruct((tiles, share, cols), F32),
        in_specs=[hbm, hbm, smem, hbm, smem],
        out_specs=vmem,
        scratch_shapes=scratch,
        compiler_params=pltpu.CompilerParams(
            collective_id=0, has_side_effects=True, vmem_limit_bytes=60 * 1024 * 1024
        ),
    )(
        factor_blocks[0],
        block_inverses[0],
        jnp.transpose(band_offsets, (2, 0, 1)),
        coupling[0],
        tile_ids.T,
    )
    return interface_block - contribution[None]


def solution(mesh):
    return jax.shard_map(
        functools.partial(shards, mesh.shape["sub"], mesh.shape["row"]),
        mesh=mesh,
        in_specs=(
            P("sub", "row", None, None, None),
            P("sub", "row", None, None),
            P("sub", "row", None),
            P("sub", "row", None),
            P("sub", None, "row", None),
            P(),
        ),
        out_specs=P("sub", None, "row", None),
        check_vma=False,
    )
```

```python
import functools

import jax
import jax.numpy as jnp
from jax import lax
from jax.experimental import pallas as pl
from jax.experimental.pallas import tpu as pltpu
from jax.sharding import PartitionSpec as P

MESH = pl.DeviceIdType.MESH
F32 = jnp.float32
BF16 = jnp.bfloat16
CHUNK = 16
NT = (((1,), (1,)), ((), ()))
NN = (((1,), (0,)), ((), ()))


def split(value):
    high = value.astype(BF16)
    low = (value - high.astype(F32)).astype(BF16)
    return high, low


def dot(a, b, dims):
    return lax.dot_general(a, b, dims, preferred_element_type=F32)


def dot3(ah, al, bh, bl, dims=NT):
    return dot(ah, bh, dims) + dot(ah, bl, dims) + dot(al, bh, dims)


def kernel(
    subs,
    rows,
    factor_hbm,
    inverse_hbm,
    offsets,
    coupling_hbm,
    tile_ids,
    out,
    factor,
    inverse,
    coupling,
    nh,
    nl,
    ih,
    il,
    yt,
    yh,
    yl,
    wh,
    wl,
    arrived,
    gpart,
    grecv,
    gsum,
    gsum_early,
    perm,
    shared,
    nearby,
    load_sem,
    chain_send,
    chain_recv,
    gram_send,
    gram_recv,
    stage_send,
    stage_recv,
    near_send,
    near_recv,
    go,
):
    sub = lax.axis_index("sub")
    row = lax.axis_index("row")
    brows, kband, block, _ = factor.shape
    height, cols = coupling.shape
    chunks = cols // CHUNK
    tiles = tile_ids.shape[0]
    tile = cols // tiles
    share = tile // rows
    half = rows // 2
    parity = lax.rem(row, 2)
    odd = parity == 1
    mine = row // 2
    piece = tiles * share
    lanes = 2 * piece
    parts = cols // lanes
    last = row == rows - 1

    loads = [
        pltpu.make_async_copy(source, target, load_sem.at[i])
        for i, (source, target) in enumerate(
            ((inverse_hbm, inverse), (coupling_hbm, coupling), (factor_hbm, factor))
        )
    ]
    for load in loads:
        load.start()

    nearby[...] = jnp.zeros_like(nearby)

    barrier = pltpu.get_barrier_semaphore()
    for step in range(1, rows):
        pl.semaphore_signal(
            barrier, inc=1, device_id=(sub, lax.rem(row + step, rows)), device_id_type=MESH
        )
    has_left = sub > 0
    has_right = sub < subs - 1

    @pl.when(has_left)
    def _():
        pl.semaphore_signal(barrier, inc=1, device_id=(sub - 1, row), device_id_type=MESH)

    @pl.when(has_right)
    def _():
        pl.semaphore_signal(barrier, inc=1, device_id=(sub + 1, row), device_id_type=MESH)

    def span(r):
        return slice(r * block, (r + 1) * block)

    def own(r):
        return slice(height + r * block, height + (r + 1) * block)

    def at_offset(r, offset):
        value = jnp.zeros((block, block), F32)
        for band in range(kband):
            if band + 1 <= offset <= band + 2:
                value = jnp.where(offsets[band, 0, r] == offset, factor[r, band], value)
        return value

    def local(r, offset):
        return r * (r - 1) // 2 + offset - 1

    loads[0].wait()
    for r in range(brows):
        high, low = split(inverse[r])
        ih[r] = high
        il[r] = low
    loads[1].wait()
    order = [
        k * tile + (2 * j + p) * share for p in range(2) for j in range(half) for k in range(tiles)
    ]
    for r in range(brows):
        natural = coupling[span(r), :].T
        high, low = split(jnp.concatenate([natural[n : n + share] for n in order], 0))
        yt[:, span(r)] = dot3(high, low, ih[r], il[r])
    loads[2].wait()
    for r in range(1, brows):
        for offset in range(1, r + 1):
            high, low = split(at_offset(r, offset))
            high, low = split(dot3(ih[r], il[r], high, low, NN))
            nh[local(r, offset)] = high
            nl[local(r, offset)] = low

    for r in range(brows):
        solved = yt[:, span(r)]
        for offset in range(r, 0, -1):
            s = own(r - offset)
            n = local(r, offset)
            solved = solved - dot3(yh[:, s], yl[:, s], nh[n], nl[n])
        if r > 0:
            yt[:, span(r)] = solved
        high, low = split(solved)
        yh[:, own(r)] = high
        yl[:, own(r)] = low

    pl.semaphore_wait(
        barrier, rows - 1 + has_left.astype(jnp.int32) + has_right.astype(jnp.int32)
    )

    following = lax.rem(row + 1, rows)

    def rows_of(c):
        return pl.ds(pl.multiple_of(c * CHUNK, CHUNK), CHUNK)

    def chain_copy(c):
        return pltpu.make_async_remote_copy(
            src_ref=yt.at[rows_of(c)],
            dst_ref=arrived.at[rows_of(c)],
            send_sem=chain_send.at[c],
            recv_sem=chain_recv.at[c],
            device_id=(sub, following),
            device_id_type=MESH,
        )

    def gram_of(start, count, part, width, depth):
        high = yh[start : start + count, depth:]
        low = yl[start : start + count, depth:]
        at = slice(part * lanes, part * lanes + width)
        both = dot(jnp.concatenate([high, low], 0), yh[at, depth:], NT)
        return both[:count] + (both[count:] + dot(high, yl[at, depth:], NT))

    def keep(gram, slot, part):
        for j in range(gram.shape[0] // piece):
            for m in range(gram.shape[1] // lanes):
                gpart[slot + j, part + m] = gram[
                    j * piece : (j + 1) * piece, m * lanes : (m + 1) * lanes
                ]

    def gram_copy(step):
        to = lax.rem(mine + step, half)
        return pltpu.make_async_remote_copy(
            src_ref=gpart.at[to],
            dst_ref=grecv.at[mine],
            send_sem=gram_send.at[step],
            recv_sem=gram_recv.at[mine],
            device_id=(sub, 2 * to + parity),
            device_id_type=MESH,
        )

    def stage_copy(q, j):
        even = j % 2 == 0
        if even:
            at = pl.ds(0, 2) if q == 1 else pl.ds(q, 1)
        else:
            first = (half + j // 2) // 2
            at = pl.ds(0, q + 1) if q == first else pl.ds(q, 1)
        return pltpu.make_async_remote_copy(
            src_ref=gpart.at[j // 2 + (half if even else 0), at],
            dst_ref=grecv.at[half if even else half - 1, at],
            send_sem=stage_send.at[q, j],
            recv_sem=stage_recv.at[q],
            device_id=(sub, j),
            device_id_type=MESH,
        )

    far_first = sorted(range(0, rows, 2), key=lambda j: -min(half - 1 - j // 2, j // 2 + 1))

    def targets(q):
        odds = [j for j in range(1, rows - 1, 2) if (half + j // 2) // 2 <= q]
        return (far_first if q > 0 else []), odds

    def send_stage(q, pieces):
        for j in pieces:
            stage_copy(q, j).start()

    def gram_stage(q):
        own_rows = half * piece
        evens, odds = targets(q)
        if q == 1:
            keep(gram_of(0, own_rows, 0, 2 * lanes, height), half, 0)
        else:
            keep(gram_of(0, own_rows, q, lanes, height), half, q)
        send_stage(q, evens)
        if q == 2:
            keep(gram_of(own_rows, lanes, 0, (q + 1) * lanes, 0), 0, 0)
            send_stage(q, odds)
        if q == 3:
            keep(gram_of(own_rows + lanes, lanes, 0, cols, 0), 2, 0)
            send_stage(q, odds[-1:])
            keep(gram_of(own_rows, lanes, q, lanes, 0), 0, q)
            send_stage(q, odds[:-1])

    @pl.when(row == 0)
    def _():
        @pl.loop(0, chunks)
        def _(c):
            chain_copy(c).start()

        yh[:, :height] = jnp.zeros((cols, height), BF16)
        yl[:, :height] = jnp.zeros((cols, height), BF16)

    @pl.when(row > 0)
    def _():
        for b in range(brows):
            for r in range(b + 1):
                high, low = split(-at_offset(r, brows + r - b).T)
                wh[span(b), span(r)] = high
                wl[span(b), span(r)] = low
        for b0 in range(0, brows, 2):
            k = slice(b0 * block, (b0 + 2) * block)
            for r in range(brows):
                solved = None
                first = max(r, b0)
                if first < b0 + 2:
                    part = slice(first * block, (b0 + 2) * block)
                    solved = dot3(wh[part, span(r)], wl[part, span(r)], ih[r], il[r])
                    if first > b0:
                        solved = jnp.concatenate(
                            [jnp.zeros(((first - b0) * block, block), F32), solved], 0
                        )
                for offset in range(r, 0, -1):
                    s = span(r - offset)
                    n = local(r, offset)
                    term = dot3(wh[k, s], wl[k, s], nh[n], nl[n])
                    solved = -term if solved is None else solved - term
                high, low = split(solved)
                wh[k, span(r)] = high
                wl[k, span(r)] = low

        @pl.loop(0, chunks)
        def _(c):
            chain_copy(c).wait_recv()
            here = rows_of(c)
            high, low = split(arrived[here, :])
            both = dot(jnp.concatenate([high, low], 0), wh[...], NN)
            value = yt[here, :] + (both[:CHUNK] + (both[CHUNK:] + dot(high, wl[...], NN)))
            yt[here, :] = value

            @pl.when(row < rows - 1)
            def _():
                chain_copy(c).start()

            yh[here, :height] = high
            yl[here, :height] = low
            high, low = split(value)
            yh[here, height:] = high
            yl[here, height:] = low

            for q in range(1, parts - 1):
                @pl.when(last & (c == (q + 1) * (chunks // parts) - 1))
                def _():
                    gram_stage(q)

    @pl.when(last)
    def _():
        gram_stage(parts - 1)

    def release(source, to):
        @pl.when(row == source)
        def _():
            pl.semaphore_signal(go, inc=1, device_id=(sub, to), device_id_type=MESH)

    release(rows - 2, rows - 4)
    for to in range(rows - 4):
        release(rows - 3 if to % 2 else rows - 4, to)

    def send_gram(source, steps):
        @pl.when(row == source)
        def _():
            for step in steps:
                gram_copy(step).start()

    def gram_half(h):
        for p in range(2):
            @pl.when((parity == p) & (row < rows - 1))
            def _():
                keep(gram_of(p * half * piece + h * lanes, lanes, 0, cols, 0), 2 * h, 0)

    gram_half(0)
    send_gram(rows - 2, (2, 1))
    send_gram(rows - 3, (2, 3))
    send_gram(rows - 4, (3,))
    gram_half(1)
    send_gram(rows - 2, (3,))
    send_gram(rows - 3, (1,))

    @pl.when(row < rows - 3)
    def _():
        pl.semaphore_wait(go, 1)

    send_gram(rows - 4, (2, 1))

    @pl.when(row < rows - 4)
    def _():
        for step in range(1, half):
            gram_copy(step).start()

    def common(owner, other):
        first = jnp.int32(tiles - 1)
        second = jnp.int32(0)
        for k in range(tiles - 1, -1, -1):
            number = tile_ids[k, owner]
            hit = number == tile_ids[0, other]
            for m in range(1, tiles):
                hit = hit | (number == tile_ids[m, other])
            first = jnp.where(hit, k, first)
        for k in range(tiles):
            number = tile_ids[k, owner]
            hit = number == tile_ids[0, other]
            for m in range(1, tiles):
                hit = hit | (number == tile_ids[m, other])
            second = jnp.where(hit, k, second)
        return first, second

    left = jnp.maximum(sub - 1, 0)
    right = jnp.minimum(sub + 1, subs - 1)

    pairs = [common(sub, right), common(sub, left)]
    matches = []
    for other, exists in ((left, has_left), (right, has_right)):
        first, second = common(other, sub)
        matches.append(
            [
                [
                    jnp.where((tile_ids[i, sub] == tile_ids[first, other]) & exists, 1.0, 0.0)
                    for i in range(tiles)
                ],
                [
                    jnp.where(
                        (tile_ids[i, sub] == tile_ids[second, other])
                        & exists
                        & (first != second),
                        1.0,
                        0.0,
                    )
                    for i in range(tiles)
                ],
            ]
        )

    at_row = lax.broadcasted_iota(jnp.int32, (cols, cols), 0)
    at_col = lax.broadcasted_iota(jnp.int32, (cols, cols), 1)
    place = at_row // piece
    home = (
        (at_row % piece) // share * tile
        + (2 * (place % half) + place // half) * share
        + at_row % share
    )
    perm[...] = jnp.where(home == at_col, 1.0, 0.0).astype(BF16)

    grecv[mine] = gpart[mine]

    def arrival(sem, slot, at):
        return pltpu.make_async_remote_copy(
            src_ref=gpart.at[0, at],
            dst_ref=grecv.at[slot, at],
            send_sem=gram_send.at[0],
            recv_sem=sem,
            device_id=(sub, following),
            device_id_type=MESH,
        )

    for j in range(half):
        @pl.when((j != mine) & ((j < half - 1) | (parity == 0)))
        def _():
            arrival(gram_recv.at[j], j, pl.ds(0, parts)).wait_recv()

    @pl.when(parity == 0)
    def _():
        arrival(stage_recv.at[1], half, pl.ds(0, 2)).wait_recv()
        arrival(stage_recv.at[2], half, pl.ds(2, 1)).wait_recv()

    @pl.when(odd & (row < rows - 3))
    def _():
        arrival(stage_recv.at[2], half - 1, pl.ds(0, 3)).wait_recv()

    @pl.when(odd & (row == rows - 3))
    def _():
        arrival(stage_recv.at[3], half - 1, pl.ds(0, parts)).wait_recv()

    def placed(blocks, start):
        value = jnp.concatenate(blocks, 1)
        high = value.astype(BF16)
        middle, low = split(value - high.astype(F32))
        moved = dot(
            jnp.concatenate([high, middle, low], 0),
            perm[start * lanes : (start + len(blocks)) * lanes, :],
            NN,
        )
        return moved[:piece] + (moved[piece : 2 * piece] + moved[2 * piece :])

    def summed(m):
        value = grecv[0, m]
        for j in range(1, half):
            value = value + grecv[j, m]
        return value + jnp.where(odd, 0.0, grecv[half, m])

    gsum_early[...] = placed([summed(m) for m in range(parts - 1)], 0)

    @pl.when(parity == 0)
    def _():
        arrival(stage_recv.at[3], half, pl.ds(3, 1)).wait_recv()

    @pl.when(odd & (row < rows - 3))
    def _():
        arrival(stage_recv.at[3], half - 1, pl.ds(3, 1)).wait_recv()

    moved = gsum_early[...] + placed([summed(parts - 1)], parts - 1)
    for k in range(tiles):
        for l in range(tiles):
            gsum[k * tiles + l] = moved[k * share : (k + 1) * share, l * tile : (l + 1) * tile]

    def near_copy(side):
        return pltpu.make_async_remote_copy(
            src_ref=shared.at[side],
            dst_ref=nearby.at[side],
            send_sem=near_send.at[side],
            recv_sem=near_recv.at[side],
            device_id=(sub + 1 if side == 0 else sub - 1, row),
            device_id_type=MESH,
        )

    for side, (other, exists) in enumerate(((right, has_right), (left, has_left))):
        pair = pairs[side]
        for p in range(2):
            for m in range(2):
                shared[side, 2 * p + m] = gsum[pair[p] * tiles + pair[m]]

        @pl.when(exists)
        def _():
            near_copy(side).start()

    @pl.when(has_left)
    def _():
        near_copy(0).wait_recv()

    @pl.when(has_right)
    def _():
        near_copy(1).wait_recv()

    for i in range(tiles):
        across = [
            [match[0][i] * nearby[side, m] + match[1][i] * nearby[side, 2 + m] for m in range(2)]
            for side, match in enumerate(matches)
        ]
        for j in range(tiles):
            value = gsum[i * tiles + j]
            for match, taken in zip(matches, across):
                value = value + (match[0][j] * taken[0] + match[1][j] * taken[1])
            out[i, :, j * tile : (j + 1) * tile] = value

    @pl.when(row < rows - 1)
    def _():
        @pl.loop(0, chunks)
        def _(c):
            chain_copy(c).wait_send()

        for step in range(1, half):
            gram_copy(step).wait_send()

    @pl.when(last)
    def _():
        for q in range(1, parts):
            for j in sum(targets(q), []):
                stage_copy(q, j).wait_send()

    @pl.when(has_right)
    def _():
        near_copy(0).wait_send()

    @pl.when(has_left)
    def _():
        near_copy(1).wait_send()


def shards(
    subs, rows, factor_blocks, block_inverses, band_offsets, coupling, interface_block, tile_ids
):
    brows, kband, block, _ = factor_blocks.shape[1:]
    height, cols = coupling.shape[1:]
    tiles, share, _ = interface_block.shape[1:]
    tile = cols // tiles
    piece = tiles * share
    lanes = 2 * piece
    parts = cols // lanes
    locals_ = brows * (brows - 1) // 2
    hbm = pl.BlockSpec(memory_space=pl.ANY)
    vmem = pl.BlockSpec(memory_space=pltpu.VMEM)
    smem = pl.BlockSpec(memory_space=pltpu.SMEM)
    dma = pltpu.SemaphoreType.DMA
    scratch = [
        pltpu.VMEM((brows, kband, block, block), F32),
        pltpu.VMEM((brows, block, block), F32),
        pltpu.VMEM((height, cols), F32),
        pltpu.VMEM((locals_, block, block), BF16),
        pltpu.VMEM((locals_, block, block), BF16),
        pltpu.VMEM((brows, block, block), BF16),
        pltpu.VMEM((brows, block, block), BF16),
        pltpu.VMEM((cols, height), F32),
        pltpu.VMEM((cols, 2 * height), BF16),
        pltpu.VMEM((cols, 2 * height), BF16),
        pltpu.VMEM((height, height), BF16),
        pltpu.VMEM((height, height), BF16),
        pltpu.VMEM((cols, height), F32),
        pltpu.VMEM((rows, parts, piece, lanes), F32),
        pltpu.VMEM((rows // 2 + 1, parts, piece, lanes), F32),
        pltpu.VMEM((tiles * tiles, share, tile), F32),
        pltpu.VMEM((piece, cols), F32),
        pltpu.VMEM((cols, cols), BF16),
        pltpu.VMEM((2, 4, share, tile), F32),
        pltpu.VMEM((2, 4, share, tile), F32),
        dma((3,)),
        dma((cols // CHUNK,)),
        dma((cols // CHUNK,)),
        dma((rows // 2,)),
        dma((rows // 2,)),
        dma((parts, rows)),
        dma((parts,)),
        dma((2,)),
        dma((2,)),
        pltpu.SemaphoreType.REGULAR,
    ]
    contribution = pl.pallas_call(
        functools.partial(kernel, subs, rows),
        out_shape=jax.ShapeDtypeStruct((tiles, share, cols), F32),
        in_specs=[hbm, hbm, smem, hbm, smem],
        out_specs=vmem,
        scratch_shapes=scratch,
        compiler_params=pltpu.CompilerParams(
            collective_id=0, has_side_effects=True, vmem_limit_bytes=60 * 1024 * 1024
        ),
    )(
        factor_blocks[0],
        block_inverses[0],
        jnp.transpose(band_offsets, (2, 0, 1)),
        coupling[0],
        tile_ids.T,
    )
    return interface_block - contribution[None]


def solution(mesh):
    return jax.shard_map(
        functools.partial(shards, mesh.shape["sub"], mesh.shape["row"]),
        mesh=mesh,
        in_specs=(
            P("sub", "row", None, None, None),
            P("sub", "row", None, None),
            P("sub", "row", None),
            P("sub", "row", None),
            P("sub", None, "row", None),
            P(),
        ),
        out_specs=P("sub", None, "row", None),
        check_vma=False,
    )
```

```python
import functools

import jax
import jax.numpy as jnp
from jax import lax
from jax.experimental import pallas as pl
from jax.experimental.pallas import tpu as pltpu
from jax.sharding import PartitionSpec as P

MESH = pl.DeviceIdType.MESH
F32 = jnp.float32
BF16 = jnp.bfloat16
CHUNK = 16
NT = (((1,), (1,)), ((), ()))
NN = (((1,), (0,)), ((), ()))


def split(value):
    high = value.astype(BF16)
    low = (value - high.astype(F32)).astype(BF16)
    return high, low


def dot(a, b, dims):
    return lax.dot_general(a, b, dims, preferred_element_type=F32)


def dot3(ah, al, bh, bl, dims=NT):
    return dot(ah, bh, dims) + dot(ah, bl, dims) + dot(al, bh, dims)


def kernel(
    subs,
    rows,
    factor_hbm,
    inverse_hbm,
    offsets,
    coupling_hbm,
    tile_ids,
    out,
    factor,
    inverse,
    coupling,
    nh,
    nl,
    ih,
    il,
    yt,
    yh,
    yl,
    wh,
    wl,
    arrived,
    gpart,
    grecv,
    gsum,
    gsum_early,
    perm,
    shared,
    nearby,
    load_sem,
    chain_send,
    chain_recv,
    gram_send,
    gram_recv,
    stage_send,
    stage_recv,
    near_send,
    near_recv,
    go,
):
    sub = lax.axis_index("sub")
    row = lax.axis_index("row")
    brows, kband, block, _ = factor.shape
    height, cols = coupling.shape
    chunks = cols // CHUNK
    tiles = tile_ids.shape[0]
    tile = cols // tiles
    share = tile // rows
    half = rows // 2
    parity = lax.rem(row, 2)
    odd = parity == 1
    mine = row // 2
    piece = tiles * share
    lanes = 2 * piece
    parts = cols // lanes
    last = row == rows - 1

    loads = [
        pltpu.make_async_copy(source, target, load_sem.at[i])
        for i, (source, target) in enumerate(
            ((inverse_hbm, inverse), (coupling_hbm, coupling), (factor_hbm, factor))
        )
    ]
    for load in loads:
        load.start()

    nearby[...] = jnp.zeros_like(nearby)

    barrier = pltpu.get_barrier_semaphore()
    for step in range(1, rows):
        pl.semaphore_signal(
            barrier, inc=1, device_id=(sub, lax.rem(row + step, rows)), device_id_type=MESH
        )
    has_left = sub > 0
    has_right = sub < subs - 1

    @pl.when(has_left)
    def _():
        pl.semaphore_signal(barrier, inc=1, device_id=(sub - 1, row), device_id_type=MESH)

    @pl.when(has_right)
    def _():
        pl.semaphore_signal(barrier, inc=1, device_id=(sub + 1, row), device_id_type=MESH)

    def span(r):
        return slice(r * block, (r + 1) * block)

    def own(r):
        return slice(height + r * block, height + (r + 1) * block)

    def at_offset(r, offset):
        value = jnp.zeros((block, block), F32)
        for band in range(kband):
            if band + 1 <= offset <= band + 2:
                value = jnp.where(offsets[band, 0, r] == offset, factor[r, band], value)
        return value

    def local(r, offset):
        return r * (r - 1) // 2 + offset - 1

    loads[0].wait()
    for r in range(brows):
        high, low = split(inverse[r])
        ih[r] = high
        il[r] = low
    loads[1].wait()
    order = [
        k * tile + (2 * j + p) * share for p in range(2) for j in range(half) for k in range(tiles)
    ]
    for r in range(brows):
        natural = coupling[span(r), :].T
        high, low = split(jnp.concatenate([natural[n : n + share] for n in order], 0))
        yt[:, span(r)] = dot3(high, low, ih[r], il[r])
    loads[2].wait()
    for r in range(1, brows):
        for offset in range(1, r + 1):
            high, low = split(at_offset(r, offset))
            high, low = split(dot3(ih[r], il[r], high, low, NN))
            nh[local(r, offset)] = high
            nl[local(r, offset)] = low

    for r in range(brows):
        solved = yt[:, span(r)]
        for offset in range(r, 0, -1):
            s = own(r - offset)
            n = local(r, offset)
            solved = solved - dot3(yh[:, s], yl[:, s], nh[n], nl[n])
        if r > 0:
            yt[:, span(r)] = solved
        high, low = split(solved)
        yh[:, own(r)] = high
        yl[:, own(r)] = low

    pl.semaphore_wait(
        barrier, rows - 1 + has_left.astype(jnp.int32) + has_right.astype(jnp.int32)
    )

    following = lax.rem(row + 1, rows)

    def rows_of(c):
        return pl.ds(pl.multiple_of(c * CHUNK, CHUNK), CHUNK)

    def chain_copy(c):
        return pltpu.make_async_remote_copy(
            src_ref=yt.at[rows_of(c)],
            dst_ref=arrived.at[rows_of(c)],
            send_sem=chain_send.at[c],
            recv_sem=chain_recv.at[c],
            device_id=(sub, following),
            device_id_type=MESH,
        )

    def gram_of(start, count, part, width, depth):
        high = yh[start : start + count, depth:]
        low = yl[start : start + count, depth:]
        at = slice(part * lanes, part * lanes + width)
        both = dot(jnp.concatenate([high, low], 0), yh[at, depth:], NT)
        return both[:count] + (both[count:] + dot(high, yl[at, depth:], NT))

    def keep(gram, slot, part):
        for j in range(gram.shape[0] // piece):
            for m in range(gram.shape[1] // lanes):
                gpart[slot + j, part + m] = gram[
                    j * piece : (j + 1) * piece, m * lanes : (m + 1) * lanes
                ]

    def gram_copy(step):
        to = lax.rem(mine + step, half)
        return pltpu.make_async_remote_copy(
            src_ref=gpart.at[to],
            dst_ref=grecv.at[mine],
            send_sem=gram_send.at[step],
            recv_sem=gram_recv.at[mine],
            device_id=(sub, 2 * to + parity),
            device_id_type=MESH,
        )

    def stage_copy(q, j):
        even = j % 2 == 0
        if even:
            at = pl.ds(0, 2) if q == 1 else pl.ds(q, 1)
        else:
            first = (half + j // 2) // 2
            at = pl.ds(0, q + 1) if q == first else pl.ds(q, 1)
        return pltpu.make_async_remote_copy(
            src_ref=gpart.at[j // 2 + (half if even else 0), at],
            dst_ref=grecv.at[half if even else half - 1, at],
            send_sem=stage_send.at[q, j],
            recv_sem=stage_recv.at[q],
            device_id=(sub, j),
            device_id_type=MESH,
        )

    far_first = sorted(range(0, rows, 2), key=lambda j: -min(half - 1 - j // 2, j // 2 + 1))

    def targets(q):
        odds = [j for j in range(1, rows - 1, 2) if (half + j // 2) // 2 <= q]
        return (far_first if q > 0 else []), odds

    def send_stage(q, pieces):
        for j in pieces:
            stage_copy(q, j).start()

    def gram_stage(q):
        own_rows = half * piece
        evens, odds = targets(q)
        if q == 1:
            keep(gram_of(0, own_rows, 0, 2 * lanes, height), half, 0)
        else:
            keep(gram_of(0, own_rows, q, lanes, height), half, q)
        send_stage(q, evens)
        if q == 2:
            keep(gram_of(own_rows, lanes, 0, (q + 1) * lanes, 0), 0, 0)
            send_stage(q, odds)
        if q == 3:
            keep(gram_of(own_rows + lanes, lanes, 0, cols, 0), 2, 0)
            send_stage(q, odds[-1:])
            keep(gram_of(own_rows, lanes, q, lanes, 0), 0, q)
            send_stage(q, odds[:-1])

    @pl.when(row == 0)
    def _():
        @pl.loop(0, chunks)
        def _(c):
            chain_copy(c).start()

        yh[:, :height] = jnp.zeros((cols, height), BF16)
        yl[:, :height] = jnp.zeros((cols, height), BF16)

    @pl.when(row > 0)
    def _():
        for b in range(brows):
            for r in range(b + 1):
                high, low = split(-at_offset(r, brows + r - b).T)
                wh[span(b), span(r)] = high
                wl[span(b), span(r)] = low
        for b0 in range(0, brows, 2):
            k = slice(b0 * block, (b0 + 2) * block)
            for r in range(brows):
                solved = None
                first = max(r, b0)
                if first < b0 + 2:
                    part = slice(first * block, (b0 + 2) * block)
                    solved = dot3(wh[part, span(r)], wl[part, span(r)], ih[r], il[r])
                    if first > b0:
                        solved = jnp.concatenate(
                            [jnp.zeros(((first - b0) * block, block), F32), solved], 0
                        )
                for offset in range(r, 0, -1):
                    s = span(r - offset)
                    n = local(r, offset)
                    term = dot3(wh[k, s], wl[k, s], nh[n], nl[n])
                    solved = -term if solved is None else solved - term
                high, low = split(solved)
                wh[k, span(r)] = high
                wl[k, span(r)] = low

        @pl.loop(0, chunks)
        def _(c):
            chain_copy(c).wait_recv()
            here = rows_of(c)
            high, low = split(arrived[here, :])
            both = dot(jnp.concatenate([high, low], 0), wh[...], NN)
            value = yt[here, :] + (both[:CHUNK] + (both[CHUNK:] + dot(high, wl[...], NN)))
            yt[here, :] = value

            @pl.when(row < rows - 1)
            def _():
                chain_copy(c).start()

            yh[here, :height] = high
            yl[here, :height] = low
            high, low = split(value)
            yh[here, height:] = high
            yl[here, height:] = low

            for q in range(1, parts - 1):
                @pl.when(last & (c == (q + 1) * (chunks // parts) - 1))
                def _():
                    gram_stage(q)

    @pl.when(last)
    def _():
        gram_stage(parts - 1)

    def release(source, to):
        @pl.when(row == source)
        def _():
            pl.semaphore_signal(go, inc=1, device_id=(sub, to), device_id_type=MESH)

    release(rows - 2, rows - 4)
    for to in range(rows - 4):
        release(rows - 3 if to % 2 else rows - 4, to)

    def send_gram(source, steps):
        @pl.when(row == source)
        def _():
            for step in steps:
                gram_copy(step).start()

    def gram_half(h):
        for p in range(2):
            @pl.when((parity == p) & (row < rows - 1))
            def _():
                keep(gram_of(p * half * piece + h * lanes, lanes, 0, cols, 0), 2 * h, 0)

    gram_half(0)
    send_gram(rows - 2, (2, 1))
    send_gram(rows - 3, (2, 3))
    send_gram(rows - 4, (3,))
    gram_half(1)
    send_gram(rows - 2, (3,))
    send_gram(rows - 3, (1,))

    @pl.when(row < rows - 3)
    def _():
        pl.semaphore_wait(go, 1)

    send_gram(rows - 4, (2, 1))

    @pl.when(row < rows - 4)
    def _():
        for step in range(1, half):
            gram_copy(step).start()

    def common(owner, other):
        first = jnp.int32(tiles - 1)
        second = jnp.int32(0)
        for k in range(tiles - 1, -1, -1):
            number = tile_ids[k, owner]
            hit = number == tile_ids[0, other]
            for m in range(1, tiles):
                hit = hit | (number == tile_ids[m, other])
            first = jnp.where(hit, k, first)
        for k in range(tiles):
            number = tile_ids[k, owner]
            hit = number == tile_ids[0, other]
            for m in range(1, tiles):
                hit = hit | (number == tile_ids[m, other])
            second = jnp.where(hit, k, second)
        return first, second

    left = jnp.maximum(sub - 1, 0)
    right = jnp.minimum(sub + 1, subs - 1)

    pairs = [common(sub, right), common(sub, left)]
    matches = []
    for other, exists in ((left, has_left), (right, has_right)):
        first, second = common(other, sub)
        matches.append(
            [
                [
                    jnp.where((tile_ids[i, sub] == tile_ids[first, other]) & exists, 1.0, 0.0)
                    for i in range(tiles)
                ],
                [
                    jnp.where(
                        (tile_ids[i, sub] == tile_ids[second, other])
                        & exists
                        & (first != second),
                        1.0,
                        0.0,
                    )
                    for i in range(tiles)
                ],
            ]
        )

    at_row = lax.broadcasted_iota(jnp.int32, (cols, cols), 0)
    at_col = lax.broadcasted_iota(jnp.int32, (cols, cols), 1)
    place = at_row // piece
    home = (
        (at_row % piece) // share * tile
        + (2 * (place % half) + place // half) * share
        + at_row % share
    )
    perm[...] = jnp.where(home == at_col, 1.0, 0.0).astype(BF16)

    grecv[mine] = gpart[mine]

    def arrival(sem, slot, at):
        return pltpu.make_async_remote_copy(
            src_ref=gpart.at[0, at],
            dst_ref=grecv.at[slot, at],
            send_sem=gram_send.at[0],
            recv_sem=sem,
            device_id=(sub, following),
            device_id_type=MESH,
        )

    for j in range(half):
        @pl.when((j != mine) & ((j < half - 1) | (parity == 0)))
        def _():
            arrival(gram_recv.at[j], j, pl.ds(0, parts)).wait_recv()

    @pl.when(parity == 0)
    def _():
        arrival(stage_recv.at[1], half, pl.ds(0, 2)).wait_recv()
        arrival(stage_recv.at[2], half, pl.ds(2, 1)).wait_recv()

    @pl.when(odd & (row < rows - 3))
    def _():
        arrival(stage_recv.at[2], half - 1, pl.ds(0, 3)).wait_recv()

    @pl.when(odd & (row == rows - 3))
    def _():
        arrival(stage_recv.at[3], half - 1, pl.ds(0, parts)).wait_recv()

    def placed(blocks, start):
        value = jnp.concatenate(blocks, 1)
        high = value.astype(BF16)
        middle, low = split(value - high.astype(F32))
        moved = dot(
            jnp.concatenate([high, middle, low], 0),
            perm[start * lanes : (start + len(blocks)) * lanes, :],
            NN,
        )
        return moved[:piece] + (moved[piece : 2 * piece] + moved[2 * piece :])

    def summed(m):
        value = grecv[0, m]
        for j in range(1, half):
            value = value + grecv[j, m]
        return value + jnp.where(odd, 0.0, grecv[half, m])

    gsum_early[...] = placed([summed(m) for m in range(parts - 1)], 0)

    @pl.when(parity == 0)
    def _():
        arrival(stage_recv.at[3], half, pl.ds(3, 1)).wait_recv()

    @pl.when(odd & (row < rows - 3))
    def _():
        arrival(stage_recv.at[3], half - 1, pl.ds(3, 1)).wait_recv()

    moved = gsum_early[...] + placed([summed(parts - 1)], parts - 1)
    for k in range(tiles):
        for l in range(tiles):
            gsum[k * tiles + l] = moved[k * share : (k + 1) * share, l * tile : (l + 1) * tile]

    def near_copy(side):
        return pltpu.make_async_remote_copy(
            src_ref=shared.at[side],
            dst_ref=nearby.at[side],
            send_sem=near_send.at[side],
            recv_sem=near_recv.at[side],
            device_id=(sub + 1 if side == 0 else sub - 1, row),
            device_id_type=MESH,
        )

    for side, (other, exists) in enumerate(((right, has_right), (left, has_left))):
        pair = pairs[side]
        for p in range(2):
            for m in range(2):
                shared[side, 2 * p + m] = gsum[pair[p] * tiles + pair[m]]

        @pl.when(exists)
        def _():
            near_copy(side).start()

    @pl.when(has_left)
    def _():
        near_copy(0).wait_recv()

    @pl.when(has_right)
    def _():
        near_copy(1).wait_recv()

    for i in range(tiles):
        across = [
            [match[0][i] * nearby[side, m] + match[1][i] * nearby[side, 2 + m] for m in range(2)]
            for side, match in enumerate(matches)
        ]
        for j in range(tiles):
            value = gsum[i * tiles + j]
            for match, taken in zip(matches, across):
                value = value + (match[0][j] * taken[0] + match[1][j] * taken[1])
            out[i, :, j * tile : (j + 1) * tile] = value

    @pl.when(row < rows - 1)
    def _():
        @pl.loop(0, chunks)
        def _(c):
            chain_copy(c).wait_send()

        for step in range(1, half):
            gram_copy(step).wait_send()

    @pl.when(last)
    def _():
        for q in range(1, parts):
            for j in sum(targets(q), []):
                stage_copy(q, j).wait_send()

    @pl.when(has_right)
    def _():
        near_copy(0).wait_send()

    @pl.when(has_left)
    def _():
        near_copy(1).wait_send()


def shards(
    subs, rows, factor_blocks, block_inverses, band_offsets, coupling, interface_block, tile_ids
):
    brows, kband, block, _ = factor_blocks.shape[1:]
    height, cols = coupling.shape[1:]
    tiles, share, _ = interface_block.shape[1:]
    tile = cols // tiles
    piece = tiles * share
    lanes = 2 * piece
    parts = cols // lanes
    locals_ = brows * (brows - 1) // 2
    hbm = pl.BlockSpec(memory_space=pl.ANY)
    vmem = pl.BlockSpec(memory_space=pltpu.VMEM)
    smem = pl.BlockSpec(memory_space=pltpu.SMEM)
    dma = pltpu.SemaphoreType.DMA
    scratch = [
        pltpu.VMEM((brows, kband, block, block), F32),
        pltpu.VMEM((brows, block, block), F32),
        pltpu.VMEM((height, cols), F32),
        pltpu.VMEM((locals_, block, block), BF16),
        pltpu.VMEM((locals_, block, block), BF16),
        pltpu.VMEM((brows, block, block), BF16),
        pltpu.VMEM((brows, block, block), BF16),
        pltpu.VMEM((cols, height), F32),
        pltpu.VMEM((cols, 2 * height), BF16),
        pltpu.VMEM((cols, 2 * height), BF16),
        pltpu.VMEM((height, height), BF16),
        pltpu.VMEM((height, height), BF16),
        pltpu.VMEM((cols, height), F32),
        pltpu.VMEM((rows, parts, piece, lanes), F32),
        pltpu.VMEM((rows // 2 + 1, parts, piece, lanes), F32),
        pltpu.VMEM((tiles * tiles, share, tile), F32),
        pltpu.VMEM((piece, cols), F32),
        pltpu.VMEM((cols, cols), BF16),
        pltpu.VMEM((2, 4, share, tile), F32),
        pltpu.VMEM((2, 4, share, tile), F32),
        dma((3,)),
        dma((cols // CHUNK,)),
        dma((cols // CHUNK,)),
        dma((rows // 2,)),
        dma((rows // 2,)),
        dma((parts, rows)),
        dma((parts,)),
        dma((2,)),
        dma((2,)),
        pltpu.SemaphoreType.REGULAR,
    ]
    contribution = pl.pallas_call(
        functools.partial(kernel, subs, rows),
        out_shape=jax.ShapeDtypeStruct((tiles, share, cols), F32),
        in_specs=[hbm, hbm, smem, hbm, smem],
        out_specs=vmem,
        scratch_shapes=scratch,
        compiler_params=pltpu.CompilerParams(
            collective_id=0, has_side_effects=True, vmem_limit_bytes=53 * 1024 * 1024
        ),
    )(
        factor_blocks[0],
        block_inverses[0],
        jnp.transpose(band_offsets, (2, 0, 1)),
        coupling[0],
        tile_ids.T,
    )
    return interface_block - contribution[None]


def solution(mesh):
    return jax.shard_map(
        functools.partial(shards, mesh.shape["sub"], mesh.shape["row"]),
        mesh=mesh,
        in_specs=(
            P("sub", "row", None, None, None),
            P("sub", "row", None, None),
            P("sub", "row", None),
            P("sub", "row", None),
            P("sub", None, "row", None),
            P(),
        ),
        out_specs=P("sub", None, "row", None),
        check_vma=False,
    )
```
